256 devices in a mesh: ctx: 32 (over y_hi, z, core), tp: 8 (over y_lo, x).
Axes of the slice: x: 4, y: 4 (y_hi: 2, y_lo: 2; y = y_hi * 2 + y_lo), z: 8, core: 2. Of those that a mesh axis runs over, the one named last changes fastest.
Arguments:
- tokens: bfloat16 [8192, 8192], P(('ctx', 'tp')), may hold values from -64 to 64
- query_weight: bfloat16 [8192, 4096], P(None, 'tp'), may hold values from -0.0625 to 0.0625
- keyval_weight: bfloat16 [8192, 2048], P(None, 'tp'), may hold values from -0.0625 to 0.0625
- doc_lengths: int32 [64], replicated, may hold values from 1 to 2048, 8192 in all
- owners: int32 [512], replicated, may hold values from 0 to 31, as said below
Outputs:
- attended: bfloat16 [8192, 4096], P('ctx', 'tp')
The draws below stay inside these ranges and needn't reach their ends.
Inputs may be any that keep to these rules, and one draw needn't show every extreme that they name: The 16 blocks of one index of ctx (blocks i * 16 to (i + 1) * 16 - 1) go to 16 different owners; for each position j < 16, the blocks i * 16 + j of all indices i go to all different owners, so every owner receives exactly one block of each position.
All inputs are finite; a program needn't handle non-finite values.
Results may differ from the reference program's by a relative error of at most 0.0055.
The reference program's roundings to bfloat16 on the way count: a program that leaves them out, or rounds other values in their place, can miss the bound.
Values may be sent and summed in bfloat16 or wider, within the bound.
A program may use at most 128 MiB of HBM per device.

```python
import math
import jax
import jax.numpy as jnp
import numpy as np
from jax import lax

D = 8192
HD = 128
HEADS = 4
QW = 4096
TOKENS = 8192
BLOCKS_DEV = 16
BLOCKS = 512
NDOC = 64
DOC_MOST = 2048
N_TP = 8


def draw_tokens(key, part):
    first = jax.random.fold_in(jax.random.fold_in(key, 7), 0)
    values = jnp.clip(jax.random.normal(first, (TOKENS, D), jnp.float32), -6.0, 6.0)
    return values.astype(jnp.bfloat16)


def draw_owners(key, part):
    cycle_count = BLOCKS // BLOCKS_DEV
    first, second = jax.random.split(jax.random.fold_in(key, 11))
    shuffle = jax.random.permutation(first, cycle_count)
    inverse = jnp.argsort(shuffle)
    offsets = jax.random.permutation(second, cycle_count)[:BLOCKS_DEV]
    chosen = shuffle[(inverse[:, None] + offsets[None, :]) % cycle_count]
    return chosen.reshape(BLOCKS).astype(jnp.int32)


def level_of(rng, shape, cuts, least, high):
    factor_of = 1.0
    for position, shards_of in cuts:
        heights = jax.random.uniform(jax.random.fold_in(jax.random.fold_in(rng, 6), position), (shards_of,), jnp.float32, least / len(cuts), high / len(cuts))
        factor_of = factor_of * jnp.repeat(jnp.exp(heights), shape[position] // shards_of).reshape((-1,) + (1,) * (len(shape) - 1 - position))
    return factor_of


def length_profile(count, total, limit, slope):
    loads = [(1 << 20) // math.isqrt(standing ** slope) + 1 for standing in range(2, count + 1)]
    surplus, counts = total - limit - (count - 1), [1] * (count - 1)
    while surplus > 0:
        movable = [i for i in range(count - 1) if counts[i] < limit]
        mass, budget = sum([loads[i] for i in movable]), surplus
        for i in movable:
            more = min(limit - counts[i], max(1, budget * loads[i] // mass), surplus)
            counts[i] = counts[i] + more
            surplus = surplus - more
    return np.array([limit] + counts)


def ragged(key, number_of, total, most, skew):
    if number_of == 2:
        one = jax.random.randint(key, (), max(1, total - most), min(most, total - 1) + 1)
        return jnp.stack([one, total - one])
    lengths = jnp.asarray(length_profile(number_of, total, most, skew), jnp.int32)
    pairs = (number_of - 1) // 2
    giver, sink = lengths[1:1 + 2 * pairs:2], lengths[2:2 + 2 * pairs:2]
    margin = jnp.minimum(giver - 1, most - sink)
    shifted = jax.random.randint(jax.random.fold_in(key, 1), (pairs,), 0, 1 << 20) % (margin + 1)
    lengths = lengths.at[1:1 + 2 * pairs:2].set(giver - shifted).at[2:2 + 2 * pairs:2].set(sink + shifted)
    return lengths[jax.random.permutation(jax.random.fold_in(key, 2), number_of)]


def bell_draw(stream_key, shape, deviation, bound, shards=(), held_as=jnp.bfloat16):
    level = level_of(stream_key, shape, shards, -0.22, 0.18) if shards else 1.0
    array = jax.random.normal(stream_key, shape, jnp.float32) * deviation * level
    return jnp.minimum(jnp.maximum(array, -bound), bound).astype(held_as)


def setup_inputs(seed: int = 0) -> dict:
    streams_of = jax.random.split(jax.random.key(seed), 6)
    return {
        "tokens": draw_tokens(jax.random.fold_in(streams_of[5], 71), 0),
        "query_weight": bell_draw(streams_of[1], (D, QW), D ** -0.5, 0.0625, ((1, 8),)),
        "keyval_weight": bell_draw(streams_of[2], (D, 2 * HD * N_TP), D ** -0.5, 0.0625, ((1, 8),)),
        "doc_lengths": ragged(streams_of[3], NDOC, TOKENS, DOC_MOST, 2).astype(jnp.int32),
        "owners": draw_owners(jax.random.fold_in(streams_of[5], 71), 0),
    }


NEG_FILL = -1e+30

def reference(tokens, query_weight, keyval_weight, doc_lengths, owners):
    total = tokens.shape[0]
    head_dim = HD
    heads = HEADS
    queries = jnp.dot(tokens, query_weight, preferred_element_type=jnp.float32).astype(jnp.bfloat16)
    keyvals = jnp.dot(tokens, keyval_weight, preferred_element_type=jnp.float32).astype(jnp.bfloat16)
    doc_ends = jnp.cumsum(doc_lengths).astype(jnp.int32)
    token_place = jnp.arange(total, dtype=jnp.int32)
    token_docs = lax.optimization_barrier(jnp.sum((doc_ends[None, :] <= token_place[:, None]).astype(jnp.int32), axis=1))
    block_rows = math.gcd(total, 512)
    score_scale = 1.0 / math.sqrt(head_dim)
    starts = jnp.arange(total // block_rows, dtype=jnp.int32) * block_rows
    outputs = []
    for group in range(N_TP):
        group_queries = queries[:, group * heads * head_dim:(group + 1) * heads * head_dim]
        key_rows = keyvals[:, 2 * head_dim * group:2 * head_dim * group + head_dim].astype(jnp.float32)
        value_rows = keyvals[:, 2 * head_dim * group + head_dim:2 * head_dim * (group + 1)].astype(jnp.float32)

        def attend(first_row):
            query_rows = lax.dynamic_slice_in_dim(group_queries, first_row, block_rows, 0).astype(jnp.float32)
            query_rows = query_rows.reshape(block_rows, heads, head_dim)
            query_place = lax.dynamic_slice_in_dim(token_place, first_row, block_rows, 0)
            query_docs = lax.dynamic_slice_in_dim(token_docs, first_row, block_rows, 0)
            allowed = (query_docs[:, None] == token_docs[None, :]) & (token_place[None, :] <= query_place[:, None])
            scores = jnp.einsum('qhd,kd->hqk', query_rows, key_rows) * score_scale
            scores = jnp.where(allowed[None], scores, NEG_FILL)
            highest = lax.optimization_barrier(jnp.max(scores, axis=2))
            weights = jnp.where(allowed[None], jnp.exp(scores - highest[:, :, None]), 0.0)
            totals = lax.optimization_barrier(jnp.sum(weights, axis=2))
            rounded = weights.astype(jnp.bfloat16).astype(jnp.float32)
            summed = jnp.einsum('hqk,kd->hqd', rounded, value_rows)
            result = summed / totals[:, :, None]
            return result.transpose(1, 0, 2).reshape(block_rows, heads * head_dim).astype(jnp.bfloat16)
        outputs.append(lax.map(attend, starts).reshape(total, heads * head_dim))
    head_out = jnp.concatenate(outputs, axis=1)
    block_count = owners.shape[0]
    block_len = total // block_count
    block_order = jnp.argsort(owners, stable=True).astype(jnp.int32)
    row_index = (block_order[:, None] * block_len + jnp.arange(block_len, dtype=jnp.int32)[None, :]).reshape(total)
    return head_out[row_index]
```

```python
import functools
import math

import jax
import jax.numpy as jnp
from jax import lax
from jax.experimental import pallas as pl
from jax.experimental.pallas import tpu as pltpu
from jax.sharding import PartitionSpec as P

NEG_FILL = -1e30
DOC_MOST = 2048
MESH = pl.DeviceIdType.MESH
PIECES = 4
X_FIRST = (0, 1)
Y_FIRST = (2, 3)
GO_RIGHT = (0, 2)
GO_LEFT = (1, 3)
HEAD_CHUNK = 2


def gather_kernel(cfg, tok_hbm, qw_hbm, kw_hbm, qbuf, kv_out,
                  tok, wq, wk, kvwin, load_sem, w_sem, tsend, trecv, ksend, krecv):
    n_ctx, n_x, reach, rows, share, depth, heads, hd, blk, n_docs = cfg
    me = lax.axis_index("ctx")
    g = lax.axis_index("tp")
    y = g // n_x
    x = g % n_x
    core = me % 2
    xr = (x + 1) % n_x
    xl = (x + n_x - 1) % n_x
    xo = (x + 2) % n_x
    yo = 1 - y
    chunk_rows = 2 * share
    per_dev = rows // blk
    part = depth // PIECES

    def shard_rows(yy, xx):
        return pl.ds(pl.multiple_of((xx * 2 + yy) * share, share), share)

    def group(yy, xx):
        return yy * n_x + xx

    loads = []
    for p in range(PIECES):
        c = pltpu.make_async_copy(tok_hbm.at[:, pl.ds(p * part, part)],
                                  tok.at[p, shard_rows(y, x), :], load_sem.at[p])
        c.start()
        loads.append(c)
    wloads = []
    for p in range(PIECES):
        c = pltpu.make_async_copy(kw_hbm.at[pl.ds(p * part, part), :], wk.at[p], w_sem.at[p])
        c.start()
        wloads.append(c)
        c = pltpu.make_async_copy(qw_hbm.at[pl.ds(p * part, part), :], wq.at[p],
                                  w_sem.at[PIECES + p])
        c.start()
        wloads.append(c)

    barrier = pltpu.get_barrier_semaphore()
    for gg in (group(y, xr), group(y, xl), group(yo, x)):
        pl.semaphore_signal(barrier, inc=1, device_id={"tp": gg}, device_id_type=MESH)

    for cc in ((me + 2) % n_ctx, (me + n_ctx - 2) % n_ctx, me + 1 - 2 * core):
        pl.semaphore_signal(barrier, inc=1, device_id={"ctx": cc}, device_id_type=MESH)
    pl.semaphore_wait(barrier, 6)
    for c in loads:
        c.wait()

    sent = []

    def tok_copy(gg, yy, xx, p, sem):
        where = tok.at[p, shard_rows(yy, xx), :]
        return pltpu.make_async_remote_copy(
            src_ref=where, dst_ref=where, send_sem=tsend.at[sem],
            recv_sem=trecv.at[(xx * 2 + yy) * PIECES + p],
            device_id={"tp": gg}, device_id_type=MESH)

    def send(gg, yy, xx, p):
        c = tok_copy(gg, yy, xx, p, len(sent))
        c.start()
        sent.append(c)

    def got(yy, xx, p):
        tok_copy(g, yy, xx, p, 0).wait_recv()

    right, left, over = group(y, xr), group(y, xl), group(yo, x)
    for p in Y_FIRST + X_FIRST:
        send(over, y, x, p)
    for p in X_FIRST + Y_FIRST:
        send(right, y, x, p)
        send(left, y, x, p)

    ksent = []
    chunk_x = (x, xl, xr, xo)

    def chunk_at(k):
        return pl.ds(pl.multiple_of(chunk_x[k] * chunk_rows, chunk_rows), chunk_rows)

    def kv_copy(target, src_slot, dst_slot, k, sem):
        return pltpu.make_async_remote_copy(
            src_ref=kvwin.at[src_slot, chunk_at(k), :],
            dst_ref=kvwin.at[dst_slot, chunk_at(k), :],
            send_sem=ksend.at[sem], recv_sem=krecv.at[dst_slot * 4 + k],
            device_id={"ctx": target}, device_id_type=MESH)

    def kv_send(target, src_slot, dst_slot, k):
        c = kv_copy(target, src_slot, dst_slot, k, len(ksent))
        c.start()
        ksent.append(c)

    def kv_got(slot, k):
        kv_copy(me, slot, slot, k, 0).wait_recv()

    up = (me + 2) % n_ctx
    twin = me + 1 - 2 * core

    def kv_step(step):
        for d in range(0, reach + 1):
            k = step - d
            if k < 0 or k > 3:
                continue
            slot = d * 2 + core
            if d > 0:
                kv_got(slot, k)
            if d < reach:
                kv_send(up, slot, slot + 2, k)
            kv_send(twin, slot, slot, k)

    def project(k):
        at = chunk_at(k)

        def kv_part(p, acc):
            return acc + jnp.dot(tok[p, at, :], wk[p], preferred_element_type=jnp.float32)

        kv = lax.fori_loop(0, PIECES, kv_part, jnp.zeros((chunk_rows, 2 * hd), jnp.float32))
        kvwin[core, at, :] = kv.astype(jnp.bfloat16)
        kv_step(k)

        def q_part(p, acc):
            return acc + jnp.dot(tok[p, at, :], wq[p], preferred_element_type=jnp.float32)

        q = lax.fori_loop(0, PIECES, q_part, jnp.zeros((chunk_rows, heads * hd), jnp.float32))
        q = q.astype(jnp.bfloat16)
        for h in range(heads):
            qbuf[h, at, :] = q[:, h * hd:(h + 1) * hd]

    for p in Y_FIRST:
        got(yo, x, p)
        send(right, yo, x, p)
        send(left, yo, x, p)
    for p in X_FIRST:
        got(y, xl, p)
        if p in GO_RIGHT:
            send(right, y, xl, p)
        send(over, y, xl, p)
        got(y, xr, p)
        if p in GO_LEFT:
            send(left, y, xr, p)
        send(over, y, xr, p)
    for c in wloads:
        c.wait()
    for p in X_FIRST:
        got(yo, x, p)
    project(0)
    for p in Y_FIRST:
        got(y, xl, p)
        if p in GO_RIGHT:
            send(right, y, xl, p)
        got(y, xr, p)
        if p in GO_LEFT:
            send(left, y, xr, p)
    for p in X_FIRST:
        got(y, xo, p)
        send(over, y, xo, p)
    for p in Y_FIRST:
        got(yo, xl, p)
        if p in GO_RIGHT:
            send(right, yo, xl, p)
        got(yo, xr, p)
        if p in GO_LEFT:
            send(left, yo, xr, p)
    for p in X_FIRST:
        got(yo, xl, p)
    project(1)
    for p in X_FIRST:
        got(yo, xr, p)
    project(2)
    for p in Y_FIRST:
        got(y, xo, p)
    for p in X_FIRST:
        got(yo, xo, p)
    for p in Y_FIRST:
        got(yo, xo, p)
    project(3)

    for m in range(1, reach + 1):
        kv_step(3 + m)
    for d in range(reach + 1):
        for k in range(4):
            kv_got(d * 2 + 1 - core, k)
    kv_out[...] = kvwin[...]
    for c in sent:
        c.wait_send()
    for c in ksent:
        c.wait_send()


def attend_kernel(cfg, qbuf, kvwin, doc_ref, own_ref, out_ref,
                  sbuf, mbuf, obuf, sendbuf, recvbuf, pmat, rmat, asend, arecv):
    n_ctx, n_x, reach, rows, share, depth, heads, hd, blk, n_docs = cfg
    me = lax.axis_index("ctx")
    core = me % 2
    chunk_rows = 2 * share
    per_dev = rows // blk
    barrier = pltpu.get_barrier_semaphore()

    def greet(d, carry):
        pl.semaphore_signal(barrier, inc=1, device_id={"ctx": (me + d) % n_ctx},
                            device_id_type=MESH)
        return carry

    lax.fori_loop(1, n_ctx, greet, 0)

    def place(index):
        return ((index // share) % 2) * (n_x * share) + (index // chunk_rows) * share + index % share

    row_place = me * rows + place(lax.broadcasted_iota(jnp.int32, (rows, 1), 0))

    def next_doc(d, carry):
        end, start = carry
        end = end + doc_ref[d]
        return end, jnp.where(row_place >= end, end, start)

    row_start = lax.fori_loop(0, n_docs, next_doc,
                              (jnp.int32(0), jnp.zeros((rows, 1), jnp.int32)))[1]

    lane_place = place(lax.broadcasted_iota(jnp.int32, (1, rows), 1))

    def block_owner(j, carry):
        return jnp.where(lane_place // blk == j, own_ref[me * per_dev + j], carry)

    lane_owner = lax.fori_loop(0, per_dev, block_owner, jnp.zeros((1, rows), jnp.int32))
    slot_row = lax.broadcasted_iota(jnp.int32, (n_ctx * blk, 1), 0)
    pmat[...] = jnp.where(
        (slot_row // blk == lane_owner) & (slot_row % blk == lane_place % blk), 1.0, 0.0
    ).astype(jnp.bfloat16)
    slot_lane = lax.broadcasted_iota(jnp.int32, (1, n_ctx * blk), 1)

    def source(s, carry):
        count, rank = carry
        hit = jnp.int32(0)
        for j in range(per_dev):
            hit = hit + jnp.where(own_ref[s * per_dev + j] == me, 1, 0)
        mine = (slot_lane // blk == s) & (jnp.full(slot_lane.shape, hit, jnp.int32) > 0)
        return count + hit, jnp.where(mine, count, rank)

    rank = lax.fori_loop(0, n_ctx, source,
                         (jnp.int32(0), jnp.full((1, n_ctx * blk), -1, jnp.int32)))[1]
    out_row = lax.broadcasted_iota(jnp.int32, (rows, 1), 0)
    rmat[...] = jnp.where(
        (out_row // blk == rank) & (out_row % blk == slot_lane % blk), 1.0, 0.0
    ).astype(jnp.bfloat16)

    mbuf[...] = jnp.full(mbuf.shape, NEG_FILL, jnp.float32)

    def window_slot(t):
        return ((t - core + 1) // 2) * 2 + (core + t) % 2

    def score(t):
        slot = window_slot(t)
        key_place = ((me + n_ctx - t) % n_ctx) * rows + lane_place
        allowed = (key_place >= row_start) & (key_place <= row_place)

        def one(h, carry):
            s = lax.dot_general(qbuf[h], kvwin[slot, :, 0:hd], (((1,), (1,)), ((), ())),
                                preferred_element_type=jnp.float32)
            s = jnp.where(allowed, s, NEG_FILL)
            sbuf[h, t] = s
            m = mbuf[h]
            for c in range(rows // 128):
                m = jnp.maximum(m, s[:, c * 128:(c + 1) * 128])
            mbuf[h] = m
            return carry

        lax.fori_loop(0, heads, one, 0)

    for t in range(2 * reach + 1):
        score(t)

    scale = math.log2(math.e) / math.sqrt(hd)
    half = rows // 2
    asent = []

    def finish(h, column):
        for r in range(2):
            at = pl.ds(r * half, half)
            top = jnp.max(mbuf[h, at, :], axis=1, keepdims=True)

            def step(t, carry):
                total, acc = carry
                w = jnp.exp2((sbuf[h, t, at, :] - top) * scale)
                for c in range(rows // 128):
                    total = total + w[:, c * 128:(c + 1) * 128]
                acc = acc + jnp.dot(w.astype(jnp.bfloat16), kvwin[window_slot(t), :, hd:2 * hd],
                                    preferred_element_type=jnp.float32)
                return total, acc

            total, acc = lax.fori_loop(0, 2 * reach + 1, step,
                                       (jnp.zeros((half, 128), jnp.float32),
                                        jnp.zeros((half, hd), jnp.float32)))
            value = acc / jnp.sum(total, axis=1, keepdims=True)
            obuf[at, column * hd:(column + 1) * hd] = value.astype(jnp.bfloat16)

    wide = HEAD_CHUNK * hd

    def a_copy(chunk, d):
        target = (me + d) % n_ctx
        return pltpu.make_async_remote_copy(
            src_ref=sendbuf.at[chunk, pl.ds(pl.multiple_of(target * blk, blk), blk), :],
            dst_ref=recvbuf.at[chunk, pl.ds(pl.multiple_of(me * blk, blk), blk), :],
            send_sem=asend.at[chunk * n_ctx + d], recv_sem=arecv.at[chunk * n_ctx + d],
            device_id={"ctx": target}, device_id_type=MESH)

    def a_got(chunk, d):
        source = (me + n_ctx - d) % n_ctx
        where = recvbuf.at[chunk, pl.ds(pl.multiple_of(source * blk, blk), blk), :]
        pltpu.make_async_remote_copy(
            src_ref=where, dst_ref=where,
            send_sem=asend.at[chunk * n_ctx + d], recv_sem=arecv.at[chunk * n_ctx + d],
            device_id={"ctx": source}, device_id_type=MESH).wait_recv()

    pl.semaphore_wait(barrier, n_ctx - 1)
    chunks = heads // HEAD_CHUNK
    my_slot = pl.ds(pl.multiple_of(me * blk, blk), blk)
    for chunk in range(chunks):
        for c in range(HEAD_CHUNK):
            finish(chunk * HEAD_CHUNK + c, c)
        sendbuf[chunk] = jnp.dot(pmat[...], obuf[...],
                                 preferred_element_type=jnp.float32).astype(jnp.bfloat16)

        def go(d, carry):
            a_copy(chunk, d).start()
            return carry

        lax.fori_loop(1, n_ctx, go, 0)
        recvbuf[chunk, my_slot, :] = sendbuf[chunk, my_slot, :]

    for chunk in range(chunks):
        def arrived(d, carry):
            a_got(chunk, d)
            return carry

        lax.fori_loop(1, n_ctx, arrived, 0)
        out_ref[:, chunk * wide:(chunk + 1) * wide] = jnp.dot(
            rmat[...], recvbuf[chunk], preferred_element_type=jnp.float32).astype(jnp.bfloat16)

    for chunk in range(chunks):
        def gone(d, carry):
            a_copy(chunk, d).wait_send()
            return carry

        lax.fori_loop(1, n_ctx, gone, 0)


def body(tokens, query_weight, keyval_weight, doc_lengths, owners):
    n_ctx = lax.axis_size("ctx")
    n_tp = lax.axis_size("tp")
    n_x = n_tp // 2
    share, depth = tokens.shape
    rows = share * n_tp
    hd = keyval_weight.shape[1] // 2
    heads = query_weight.shape[1] // hd
    per_dev = owners.shape[0] // n_ctx
    blk = rows // per_dev
    reach = -(-DOC_MOST // (2 * rows))
    n_docs = doc_lengths.shape[0]
    cfg = (n_ctx, n_x, reach, rows, share, depth, heads, hd, blk, n_docs)
    part = depth // PIECES
    slots = 2 * (reach + 1)
    chunks = heads // HEAD_CHUNK
    wide = HEAD_CHUNK * hd
    bf, f32 = jnp.bfloat16, jnp.float32
    n_tok = 12 + 4 * len(Y_FIRST) + 4 * len(X_FIRST) + 8
    n_kv = 4 * (2 * reach + 1)
    dma = pltpu.SemaphoreType.DMA
    q, kv = pl.pallas_call(
        functools.partial(gather_kernel, cfg),
        out_shape=(jax.ShapeDtypeStruct((heads, rows, hd), bf),
                   jax.ShapeDtypeStruct((slots, rows, 2 * hd), bf)),
        in_specs=[pl.BlockSpec(memory_space=pl.ANY)] * 3,
        out_specs=[pl.BlockSpec(memory_space=pltpu.VMEM)] * 2,
        scratch_shapes=[
            pltpu.VMEM((PIECES, rows, part), bf),
            pltpu.VMEM((PIECES, part, heads * hd), bf),
            pltpu.VMEM((PIECES, part, 2 * hd), bf),
            pltpu.VMEM((slots, rows, 2 * hd), bf),
            dma((PIECES,)),
            dma((2 * PIECES,)),
            dma((n_tok,)),
            dma((2 * n_x * PIECES,)),
            dma((n_kv,)),
            dma((slots * 4,)),
        ],
        compiler_params=pltpu.CompilerParams(
            collective_id=0, has_side_effects=True, vmem_limit_bytes=48 * 1024 * 1024
        ),
    )(tokens, query_weight, keyval_weight)
    return pl.pallas_call(
        functools.partial(attend_kernel, cfg),
        out_shape=jax.ShapeDtypeStruct((rows, heads * hd), bf),
        in_specs=[pl.BlockSpec(memory_space=pltpu.VMEM)] * 2
        + [pl.BlockSpec(memory_space=pltpu.SMEM)] * 2,
        out_specs=pl.BlockSpec(memory_space=pltpu.VMEM),
        scratch_shapes=[
            pltpu.VMEM((heads, 2 * reach + 1, rows, rows), f32),
            pltpu.VMEM((heads, rows, 128), f32),
            pltpu.VMEM((rows, wide), bf),
            pltpu.VMEM((chunks, n_ctx * blk, wide), bf),
            pltpu.VMEM((chunks, n_ctx * blk, wide), bf),
            pltpu.VMEM((n_ctx * blk, rows), bf),
            pltpu.VMEM((rows, n_ctx * blk), bf),
            dma((chunks * n_ctx,)),
            dma((chunks * n_ctx,)),
        ],
        compiler_params=pltpu.CompilerParams(
            collective_id=1, has_side_effects=True, vmem_limit_bytes=48 * 1024 * 1024
        ),
    )(q, kv, doc_lengths, owners)


def solution(mesh):
    return jax.shard_map(
        body,
        mesh=mesh,
        in_specs=(P(("ctx", "tp"), None), P(None, "tp"), P(None, "tp"), P(), P()),
        out_specs=P("ctx", "tp"),
        check_vma=False,
    )
```

```python
import functools
import math

import jax
import jax.numpy as jnp
from jax import lax
from jax.experimental import pallas as pl
from jax.experimental.pallas import tpu as pltpu
from jax.sharding import PartitionSpec as P

NEG_FILL = -1e30
DOC_MOST = 2048
MESH = pl.DeviceIdType.MESH
PIECES = 8
X_FIRST = (0, 1)
Y_FIRST = (2, 3, 4, 5, 6, 7)
GO_RIGHT = (0, 2, 4, 6)
GO_LEFT = (1, 3, 5, 7)
HEAD_CHUNK = 2


def gather_kernel(cfg, tok_hbm, qw_hbm, kw_hbm, q_out, kv_out,
                  tok, wq, wk, kvs, load_sem, w_sem, tsend, trecv, ksend, krecv):
    n_ctx, n_x, reach, rows, share, depth, heads, hd, blk, n_docs = cfg
    me = lax.axis_index("ctx")
    g = lax.axis_index("tp")
    y = g // n_x
    x = g % n_x
    core = me % 2
    xr = (x + 1) % n_x
    xl = (x + n_x - 1) % n_x
    xo = (x + 2) % n_x
    yo = 1 - y
    chunk_rows = 2 * share
    part = depth // PIECES

    def shard_rows(yy, xx):
        return pl.ds(pl.multiple_of((xx * 2 + yy) * share, share), share)

    def group(yy, xx):
        return yy * n_x + xx

    loads = []
    for p in range(PIECES):
        c = pltpu.make_async_copy(tok_hbm.at[:, pl.ds(p * part, part)],
                                  tok.at[p, shard_rows(y, x), :], load_sem.at[p])
        c.start()
        loads.append(c)
    wloads = []
    for p in range(PIECES):
        c = pltpu.make_async_copy(kw_hbm.at[pl.ds(p * part, part), :], wk.at[p], w_sem.at[p])
        c.start()
        wloads.append(c)
        c = pltpu.make_async_copy(qw_hbm.at[pl.ds(p * part, part), :], wq.at[p],
                                  w_sem.at[PIECES + p])
        c.start()
        wloads.append(c)

    barrier = pltpu.get_barrier_semaphore()
    for gg in (group(y, xr), group(y, xl), group(yo, x)):
        pl.semaphore_signal(barrier, inc=1, device_id={"tp": gg}, device_id_type=MESH)

    for cc in ((me + 2) % n_ctx, (me + n_ctx - 2) % n_ctx, me + 1 - 2 * core):
        pl.semaphore_signal(barrier, inc=1, device_id={"ctx": cc}, device_id_type=MESH)
    pl.semaphore_wait(barrier, 6)
    for c in loads:
        c.wait()

    sent = []

    def tok_copy(gg, yy, xx, p, sem):
        where = tok.at[p, shard_rows(yy, xx), :]
        return pltpu.make_async_remote_copy(
            src_ref=where, dst_ref=where, send_sem=tsend.at[sem],
            recv_sem=trecv.at[(xx * 2 + yy) * PIECES + p],
            device_id={"tp": gg}, device_id_type=MESH)

    def send(gg, yy, xx, p):
        c = tok_copy(gg, yy, xx, p, len(sent))
        c.start()
        sent.append(c)

    def got(yy, xx, p):
        tok_copy(g, yy, xx, p, 0).wait_recv()

    right, left, over = group(y, xr), group(y, xl), group(yo, x)
    for p in Y_FIRST + X_FIRST:
        send(over, y, x, p)
    for p in X_FIRST + Y_FIRST:
        send(right, y, x, p)
        send(left, y, x, p)

    for d in range(1, reach + 1):
        def clear(d=d):
            kvs[d][...] = jnp.zeros(kvs[d].shape, jnp.bfloat16)
        pl.when(me // 2 < d)(clear)

    ksent = []
    chunk_x = (x, xl, xr, xo)

    def chunk_at(k):
        return pl.ds(pl.multiple_of(chunk_x[k] * chunk_rows, chunk_rows), chunk_rows)

    def kv_copy(target, src_d, dst_d, half, k, sem):
        return pltpu.make_async_remote_copy(
            src_ref=kvs[src_d].at[half, chunk_at(k), :],
            dst_ref=kvs[dst_d].at[half, chunk_at(k), :],
            send_sem=ksend.at[sem], recv_sem=krecv.at[dst_d * 8 + half * 4 + k],
            device_id={"ctx": target}, device_id_type=MESH)

    def kv_send(target, src_d, dst_d, k, when):
        c = kv_copy(target, src_d, dst_d, core, k, len(ksent))
        pl.when(when)(c.start)
        ksent.append((c, when))

    def kv_got(d, half, k):
        kv_copy(me, d, d, half, k, 0).wait_recv()

    up = (me + 2) % n_ctx
    twin = me + 1 - 2 * core
    chip = me // 2
    last = n_ctx // 2 - 1

    def kv_step(step):
        for d in range(0, reach + 1):
            k = step - d
            if k < 0 or k > 3:
                continue
            if d > 0:
                pl.when(chip >= d)(functools.partial(kv_got, d, core, k))
            if d < reach:
                kv_send(up, d, d + 1, k, (chip >= d) & (chip < last))
            kv_send(twin, d, d, k, chip >= d)

    def project(k):
        at = chunk_at(k)

        def kv_part(p, acc):
            return acc + jnp.dot(tok[p, at, :], wk[p], preferred_element_type=jnp.float32)

        kv = lax.fori_loop(0, PIECES, kv_part, jnp.zeros((chunk_rows, 2 * hd), jnp.float32))
        kvs[0][core, at, :] = kv.astype(jnp.bfloat16)
        kv_step(k)

        def q_part(p, acc):
            return acc + jnp.dot(tok[p, at, :], wq[p], preferred_element_type=jnp.float32)

        q = lax.fori_loop(0, PIECES, q_part, jnp.zeros((chunk_rows, heads * hd), jnp.float32))
        q = q.astype(jnp.bfloat16)
        for h in range(heads):
            q_out[h, at, :] = q[:, h * hd:(h + 1) * hd]

    for p in Y_FIRST:
        got(yo, x, p)
        send(right, yo, x, p)
        send(left, yo, x, p)
    for p in X_FIRST:
        got(y, xl, p)
        if p in GO_RIGHT:
            send(right, y, xl, p)
        send(over, y, xl, p)
        got(y, xr, p)
        if p in GO_LEFT:
            send(left, y, xr, p)
        send(over, y, xr, p)
    for c in wloads:
        c.wait()
    for p in X_FIRST:
        got(yo, x, p)
    project(0)
    for p in Y_FIRST:
        got(y, xl, p)
        if p in GO_RIGHT:
            send(right, y, xl, p)
        got(y, xr, p)
        if p in GO_LEFT:
            send(left, y, xr, p)
    for p in X_FIRST:
        got(y, xo, p)
        send(over, y, xo, p)
    for p in Y_FIRST:
        got(yo, xl, p)
        if p in GO_RIGHT:
            send(right, yo, xl, p)
        got(yo, xr, p)
        if p in GO_LEFT:
            send(left, yo, xr, p)
    for p in X_FIRST:
        got(yo, xl, p)
    project(1)
    for p in X_FIRST:
        got(yo, xr, p)
    project(2)
    for p in Y_FIRST:
        got(y, xo, p)
    for p in X_FIRST:
        got(yo, xo, p)
    for p in Y_FIRST:
        got(yo, xo, p)
    project(3)

    def twin_got(d):
        for k in range(4):
            kv_got(d, 1 - core, k)

    for d in range(reach + 1):
        if d > 0:
            kv_step(3 + d)
        pl.when(chip >= d)(functools.partial(twin_got, d))
        for half in range(2):
            kv_out[(2 * d + half) * rows:(2 * d + half + 1) * rows, :] = kvs[d][half]
    for c in sent:
        c.wait_send()
    for c, when in ksent:
        pl.when(when)(c.wait_send)


def attend_kernel(cfg, qbuf, kvwin, doc_ref, own_ref, out_ref,
                  sbuf, mbuf, obuf, sendbuf, recvbuf, pmat, rmat, asend, arecv):
    n_ctx, n_x, reach, rows, share, depth, heads, hd, blk, n_docs = cfg
    me = lax.axis_index("ctx")
    core = me % 2
    chunk_rows = 2 * share
    per_dev = rows // blk
    barrier = pltpu.get_barrier_semaphore()

    def greet(d, carry):
        pl.semaphore_signal(barrier, inc=1, device_id={"ctx": (me + d) % n_ctx},
                            device_id_type=MESH)
        return carry

    lax.fori_loop(1, n_ctx, greet, 0)

    def place(index):
        return ((index // share) % 2) * (n_x * share) + (index // chunk_rows) * share + index % share

    row_place = me * rows + place(lax.broadcasted_iota(jnp.int32, (rows, 1), 0))

    def next_doc(d, carry):
        end, start = carry
        end = end + doc_ref[d]
        return end, jnp.where(row_place >= end, end, start)

    row_start = lax.fori_loop(0, n_docs, next_doc,
                              (jnp.int32(0), jnp.zeros((rows, 1), jnp.int32)))[1]

    lane_place = place(lax.broadcasted_iota(jnp.int32, (1, rows), 1))

    def block_owner(j, carry):
        return jnp.where(lane_place // blk == j, own_ref[me * per_dev + j], carry)

    lane_owner = lax.fori_loop(0, per_dev, block_owner, jnp.zeros((1, rows), jnp.int32))
    slot_row = lax.broadcasted_iota(jnp.int32, (n_ctx * blk, 1), 0)
    pmat[...] = jnp.where(
        (slot_row // blk == lane_owner) & (slot_row % blk == lane_place % blk), 1.0, 0.0
    ).astype(jnp.bfloat16)
    slot_lane = lax.broadcasted_iota(jnp.int32, (1, n_ctx * blk), 1)

    def source(s, carry):
        count, rank = carry
        hit = jnp.int32(0)
        for j in range(per_dev):
            hit = hit + jnp.where(own_ref[s * per_dev + j] == me, 1, 0)
        mine = (slot_lane // blk == s) & (jnp.full(slot_lane.shape, hit, jnp.int32) > 0)
        return count + hit, jnp.where(mine, count, rank)

    rank = lax.fori_loop(0, n_ctx, source,
                         (jnp.int32(0), jnp.full((1, n_ctx * blk), -1, jnp.int32)))[1]
    out_row = lax.broadcasted_iota(jnp.int32, (rows, 1), 0)
    rmat[...] = jnp.where(
        (out_row // blk == rank) & (out_row % blk == slot_lane % blk), 1.0, 0.0
    ).astype(jnp.bfloat16)

    scale = math.log2(math.e) / math.sqrt(hd)
    half = rows // 2
    asent = []

    span = 2 * rows
    places = jnp.concatenate([lane_place, lane_place + rows], axis=1)
    mbuf[...] = jnp.full(mbuf.shape, NEG_FILL, jnp.float32)

    def score(d, carry):
        first = ((me - core + n_ctx - 2 * d) % n_ctx) * rows
        key_place = places + first
        allowed = (key_place >= row_start) & (key_place <= row_place)
        keys = kvwin[pl.ds(pl.multiple_of(d * span, span), span), 0:hd]
        for h in range(heads):
            s = lax.dot_general(qbuf[h], keys, (((1,), (1,)), ((), ())),
                                preferred_element_type=jnp.float32)
            s = jnp.where(allowed, s, NEG_FILL)
            sbuf[h, d] = s
            m = mbuf[h]
            for j in range(span // 128):
                m = jnp.maximum(m, s[:, j * 128:(j + 1) * 128])
            mbuf[h] = m
        return carry

    lax.fori_loop(0, reach + 1, score, 0)

    def finish(chunk):
        def one(index, carry):
            c = index // 2
            h = chunk * HEAD_CHUNK + c
            at = pl.ds(pl.multiple_of((index % 2) * half, half), half)
            top = jnp.max(mbuf[h, at, :], axis=1, keepdims=True)
            total = jnp.zeros((half, 128), jnp.float32)
            acc = jnp.zeros((half, hd), jnp.float32)
            for d in range(reach + 1):
                w = jnp.exp2((sbuf[h, d, at, :] - top) * scale)
                for j in range(span // 128):
                    total = total + w[:, j * 128:(j + 1) * 128]
                acc = acc + jnp.dot(w.astype(jnp.bfloat16),
                                    kvwin[d * span:(d + 1) * span, hd:2 * hd],
                                    preferred_element_type=jnp.float32)
            value = acc / jnp.sum(total, axis=1, keepdims=True)
            obuf[c, at, :] = value.astype(jnp.bfloat16)
            return carry

        lax.fori_loop(0, 2 * HEAD_CHUNK, one, 0)

    wide = HEAD_CHUNK * hd

    def a_copy(chunk, d):
        target = (me + d) % n_ctx
        return pltpu.make_async_remote_copy(
            src_ref=sendbuf.at[chunk, pl.ds(pl.multiple_of(target * blk, blk), blk), :],
            dst_ref=recvbuf.at[chunk, pl.ds(pl.multiple_of(me * blk, blk), blk), :],
            send_sem=asend.at[chunk * n_ctx + d], recv_sem=arecv.at[chunk * n_ctx + d],
            device_id={"ctx": target}, device_id_type=MESH)

    def a_got(chunk, d):
        source = (me + n_ctx - d) % n_ctx
        where = recvbuf.at[chunk, pl.ds(pl.multiple_of(source * blk, blk), blk), :]
        pltpu.make_async_remote_copy(
            src_ref=where, dst_ref=where,
            send_sem=asend.at[chunk * n_ctx + d], recv_sem=arecv.at[chunk * n_ctx + d],
            device_id={"ctx": source}, device_id_type=MESH).wait_recv()

    pl.semaphore_wait(barrier, n_ctx - 1)
    chunks = heads // HEAD_CHUNK
    my_slot = pl.ds(pl.multiple_of(me * blk, blk), blk)
    for chunk in range(chunks):
        finish(chunk)
        for c in range(HEAD_CHUNK):
            sendbuf[chunk, :, c * hd:(c + 1) * hd] = jnp.dot(
                pmat[...], obuf[c], preferred_element_type=jnp.float32).astype(jnp.bfloat16)

        def go(d, carry):
            a_copy(chunk, d).start()
            return carry

        lax.fori_loop(1, n_ctx, go, 0)
        recvbuf[chunk, my_slot, :] = sendbuf[chunk, my_slot, :]

    for chunk in range(chunks):
        def arrived(d, carry):
            a_got(chunk, d)
            return carry

        lax.fori_loop(1, n_ctx, arrived, 0)
        out_ref[:, chunk * wide:(chunk + 1) * wide] = jnp.dot(
            rmat[...], recvbuf[chunk], preferred_element_type=jnp.float32).astype(jnp.bfloat16)

    for chunk in range(chunks):
        def gone(d, carry):
            a_copy(chunk, d).wait_send()
            return carry

        lax.fori_loop(1, n_ctx, gone, 0)


def body(tokens, query_weight, keyval_weight, doc_lengths, owners):
    n_ctx = lax.axis_size("ctx")
    n_tp = lax.axis_size("tp")
    n_x = n_tp // 2
    share, depth = tokens.shape
    rows = share * n_tp
    hd = keyval_weight.shape[1] // 2
    heads = query_weight.shape[1] // hd
    per_dev = owners.shape[0] // n_ctx
    blk = rows // per_dev
    reach = -(-DOC_MOST // (2 * rows))
    n_docs = doc_lengths.shape[0]
    cfg = (n_ctx, n_x, reach, rows, share, depth, heads, hd, blk, n_docs)
    part = depth // PIECES
    slots = 2 * (reach + 1)
    chunks = heads // HEAD_CHUNK
    wide = HEAD_CHUNK * hd
    bf, f32 = jnp.bfloat16, jnp.float32
    n_tok = 10 * PIECES
    n_kv = 4 * (2 * reach + 1)
    dma = pltpu.SemaphoreType.DMA
    q, kv = pl.pallas_call(
        functools.partial(gather_kernel, cfg),
        out_shape=(jax.ShapeDtypeStruct((heads, rows, hd), bf),
                   jax.ShapeDtypeStruct((slots * rows, 2 * hd), bf)),
        in_specs=[pl.BlockSpec(memory_space=pl.ANY)] * 3,
        out_specs=[pl.BlockSpec(memory_space=pltpu.VMEM)] * 2,
        scratch_shapes=[
            pltpu.VMEM((PIECES, rows, part), bf),
            pltpu.VMEM((PIECES, part, heads * hd), bf),
            pltpu.VMEM((PIECES, part, 2 * hd), bf),
            [pltpu.VMEM((2, rows, 2 * hd), bf) for _ in range(reach + 1)],
            dma((PIECES,)),
            dma((2 * PIECES,)),
            dma((n_tok,)),
            dma((2 * n_x * PIECES,)),
            dma((n_kv,)),
            dma((slots * 4,)),
        ],
        compiler_params=pltpu.CompilerParams(
            collective_id=0, has_side_effects=True, vmem_limit_bytes=48 * 1024 * 1024
        ),
    )(tokens, query_weight, keyval_weight)
    return pl.pallas_call(
        functools.partial(attend_kernel, cfg),
        out_shape=jax.ShapeDtypeStruct((rows, heads * hd), bf),
        in_specs=[pl.BlockSpec(memory_space=pltpu.VMEM)] * 2
        + [pl.BlockSpec(memory_space=pltpu.SMEM)] * 2,
        out_specs=pl.BlockSpec(memory_space=pltpu.VMEM),
        scratch_shapes=[
            pltpu.VMEM((heads, reach + 1, rows, 2 * rows), f32),
            pltpu.VMEM((heads, rows, 128), f32),
            pltpu.VMEM((HEAD_CHUNK, rows, hd), bf),
            pltpu.VMEM((chunks, n_ctx * blk, wide), bf),
            pltpu.VMEM((chunks, n_ctx * blk, wide), bf),
            pltpu.VMEM((n_ctx * blk, rows), bf),
            pltpu.VMEM((rows, n_ctx * blk), bf),
            dma((chunks * n_ctx,)),
            dma((chunks * n_ctx,)),
        ],
        compiler_params=pltpu.CompilerParams(
            collective_id=1, has_side_effects=True, vmem_limit_bytes=48 * 1024 * 1024
        ),
    )(q, kv, doc_lengths, owners)


def solution(mesh):
    return jax.shard_map(
        body,
        mesh=mesh,
        in_specs=(P(("ctx", "tp"), None), P(None, "tp"), P(None, "tp"), P(), P()),
        out_specs=P("ctx", "tp"),
        check_vma=False,
    )
```

```python
import functools
import math

import jax
import jax.numpy as jnp
from jax import lax
from jax.experimental import pallas as pl
from jax.experimental.pallas import tpu as pltpu
from jax.sharding import PartitionSpec as P

NEG_FILL = -1e30
DOC_MOST = 2048
MESH = pl.DeviceIdType.MESH
PIECES = 4
X_FIRST = (0,)
Y_FIRST = (1, 2, 3)
GO_RIGHT = (0, 2)
GO_LEFT = (1, 3)
HEAD_CHUNK = 2


def gather_kernel(cfg, tok_hbm, qw_hbm, kw_hbm, q_out, kv_out,
                  tok, wq, wk, kvs, load_sem, w_sem, tsend, trecv, ksend, krecv):
    n_ctx, n_x, reach, rows, share, depth, heads, hd, blk, n_docs = cfg
    me = lax.axis_index("ctx")
    g = lax.axis_index("tp")
    y = g // n_x
    x = g % n_x
    core = me % 2
    xr = (x + 1) % n_x
    xl = (x + n_x - 1) % n_x
    xo = (x + 2) % n_x
    yo = 1 - y
    chunk_rows = 2 * share
    part = depth // PIECES

    def shard_rows(yy, xx):
        return pl.ds(pl.multiple_of((xx * 2 + yy) * share, share), share)

    def group(yy, xx):
        return yy * n_x + xx

    loads = []
    for p in range(PIECES):
        c = pltpu.make_async_copy(tok_hbm.at[:, pl.ds(p * part, part)],
                                  tok.at[p, shard_rows(y, x), :], load_sem.at[p])
        c.start()
        loads.append(c)
    wloads = []
    for p in range(PIECES):
        c = pltpu.make_async_copy(kw_hbm.at[pl.ds(p * part, part), :], wk.at[p], w_sem.at[p])
        c.start()
        wloads.append(c)
        c = pltpu.make_async_copy(qw_hbm.at[pl.ds(p * part, part), :], wq.at[p],
                                  w_sem.at[PIECES + p])
        c.start()
        wloads.append(c)

    barrier = pltpu.get_barrier_semaphore()
    for gg in (group(y, xr), group(y, xl), group(yo, x)):
        pl.semaphore_signal(barrier, inc=1, device_id={"tp": gg}, device_id_type=MESH)

    for cc in ((me + 2) % n_ctx, (me + n_ctx - 2) % n_ctx, me + 1 - 2 * core):
        pl.semaphore_signal(barrier, inc=1, device_id={"ctx": cc}, device_id_type=MESH)
    pl.semaphore_wait(barrier, 6)
    for c in loads:
        c.wait()

    sent = []

    def tok_copy(gg, yy, xx, p, sem):
        where = tok.at[p, shard_rows(yy, xx), :]
        return pltpu.make_async_remote_copy(
            src_ref=where, dst_ref=where, send_sem=tsend.at[sem],
            recv_sem=trecv.at[(xx * 2 + yy) * PIECES + p],
            device_id={"tp": gg}, device_id_type=MESH)

    def send(gg, yy, xx, p):
        c = tok_copy(gg, yy, xx, p, len(sent))
        c.start()
        sent.append(c)

    def got(yy, xx, p):
        tok_copy(g, yy, xx, p, 0).wait_recv()

    right, left, over = group(y, xr), group(y, xl), group(yo, x)
    for p in Y_FIRST + X_FIRST:
        send(over, y, x, p)
    for p in X_FIRST + Y_FIRST:
        send(right, y, x, p)
        send(left, y, x, p)

    for d in range(1, reach + 1):
        def clear(d=d):
            kvs[d][...] = jnp.zeros(kvs[d].shape, jnp.bfloat16)
        pl.when(me // 2 < d)(clear)

    ksent = []
    chunk_x = (x, xl, xr, xo)

    def chunk_at(k):
        return pl.ds(pl.multiple_of(chunk_x[k] * chunk_rows, chunk_rows), chunk_rows)

    def kv_copy(target, src_d, dst_d, half, k, sem):
        return pltpu.make_async_remote_copy(
            src_ref=kvs[src_d].at[half, chunk_at(k), :],
            dst_ref=kvs[dst_d].at[half, chunk_at(k), :],
            send_sem=ksend.at[sem], recv_sem=krecv.at[dst_d * 8 + half * 4 + k],
            device_id={"ctx": target}, device_id_type=MESH)

    def kv_send(target, src_d, dst_d, k, when):
        c = kv_copy(target, src_d, dst_d, core, k, len(ksent))
        pl.when(when)(c.start)
        ksent.append((c, when))

    def kv_got(d, half, k):
        kv_copy(me, d, d, half, k, 0).wait_recv()

    up = (me + 2) % n_ctx
    twin = me + 1 - 2 * core
    chip = me // 2
    last = n_ctx // 2 - 1

    def kv_step(step):
        for d in range(0, reach + 1):
            k = step - d
            if k < 0 or k > 3:
                continue
            if d > 0:
                pl.when(chip >= d)(functools.partial(kv_got, d, core, k))
            if d < reach:
                kv_send(up, d, d + 1, k, (chip >= d) & (chip < last))
            kv_send(twin, d, d, k, chip >= d)

    def project(k):
        at = chunk_at(k)

        def kv_part(p, acc):
            return acc + jnp.dot(tok[p, at, :], wk[p], preferred_element_type=jnp.float32)

        kv = lax.fori_loop(0, PIECES, kv_part, jnp.zeros((chunk_rows, 2 * hd), jnp.float32))
        kvs[0][core, at, :] = kv.astype(jnp.bfloat16)
        kv_step(k)

        def q_part(p, acc):
            return acc + jnp.dot(tok[p, at, :], wq[p], preferred_element_type=jnp.float32)

        q = lax.fori_loop(0, PIECES, q_part, jnp.zeros((chunk_rows, heads * hd), jnp.float32))
        q = q.astype(jnp.bfloat16)
        for h in range(heads):
            q_out[h, at, :] = q[:, h * hd:(h + 1) * hd]

    for p in Y_FIRST:
        got(yo, x, p)
        send(right, yo, x, p)
        send(left, yo, x, p)
    for p in X_FIRST:
        got(y, xl, p)
        if p in GO_RIGHT:
            send(right, y, xl, p)
        send(over, y, xl, p)
        got(y, xr, p)
        if p in GO_LEFT:
            send(left, y, xr, p)
        send(over, y, xr, p)
    for c in wloads:
        c.wait()
    for p in X_FIRST:
        got(yo, x, p)
    project(0)
    for p in Y_FIRST:
        got(y, xl, p)
        if p in GO_RIGHT:
            send(right, y, xl, p)
        got(y, xr, p)
        if p in GO_LEFT:
            send(left, y, xr, p)
    for p in X_FIRST:
        got(y, xo, p)
        send(over, y, xo, p)
    for p in Y_FIRST:
        got(yo, xl, p)
        if p in GO_RIGHT:
            send(right, yo, xl, p)
        got(yo, xr, p)
        if p in GO_LEFT:
            send(left, yo, xr, p)
    for p in X_FIRST:
        got(yo, xl, p)
    project(1)
    for p in X_FIRST:
        got(yo, xr, p)
    project(2)
    for p in Y_FIRST:
        got(y, xo, p)
    for p in X_FIRST:
        got(yo, xo, p)
    for p in Y_FIRST:
        got(yo, xo, p)
    project(3)

    def twin_got(d):
        for k in range(4):
            kv_got(d, 1 - core, k)

    for d in range(reach + 1):
        if d > 0:
            kv_step(3 + d)
        pl.when(chip >= d)(functools.partial(twin_got, d))
        for half in range(2):
            kv_out[(2 * d + half) * rows:(2 * d + half + 1) * rows, :] = kvs[d][half]
    for c in sent:
        c.wait_send()
    for c, when in ksent:
        pl.when(when)(c.wait_send)


def attend_kernel(cfg, qbuf, kvwin, doc_ref, own_ref, out_ref,
                  sbuf, mbuf, obuf, sendbuf, recvbuf, pmat, rmat, asend, arecv):
    n_ctx, n_x, reach, rows, share, depth, heads, hd, blk, n_docs = cfg
    me = lax.axis_index("ctx")
    core = me % 2
    chunk_rows = 2 * share
    per_dev = rows // blk
    barrier = pltpu.get_barrier_semaphore()

    def greet(d, carry):
        pl.semaphore_signal(barrier, inc=1, device_id={"ctx": (me + d) % n_ctx},
                            device_id_type=MESH)
        return carry

    lax.fori_loop(1, n_ctx, greet, 0)

    def place(index):
        return ((index // share) % 2) * (n_x * share) + (index // chunk_rows) * share + index % share

    row_place = me * rows + place(lax.broadcasted_iota(jnp.int32, (rows, 1), 0))

    def next_doc(d, carry):
        end, start = carry
        end = end + doc_ref[d]
        return end, jnp.where(row_place >= end, end, start)

    row_start = lax.fori_loop(0, n_docs, next_doc,
                              (jnp.int32(0), jnp.zeros((rows, 1), jnp.int32)))[1]

    lane_place = place(lax.broadcasted_iota(jnp.int32, (1, rows), 1))

    def block_owner(j, carry):
        return jnp.where(lane_place // blk == j, own_ref[me * per_dev + j], carry)

    lane_owner = lax.fori_loop(0, per_dev, block_owner, jnp.zeros((1, rows), jnp.int32))
    slot_row = lax.broadcasted_iota(jnp.int32, (n_ctx * blk, 1), 0)
    pmat[...] = jnp.where(
        (slot_row // blk == lane_owner) & (slot_row % blk == lane_place % blk), 1.0, 0.0
    ).astype(jnp.bfloat16)
    slot_lane = lax.broadcasted_iota(jnp.int32, (1, n_ctx * blk), 1)

    def source(s, carry):
        count, rank = carry
        hit = jnp.int32(0)
        for j in range(per_dev):
            hit = hit + jnp.where(own_ref[s * per_dev + j] == me, 1, 0)
        mine = (slot_lane // blk == s) & (jnp.full(slot_lane.shape, hit, jnp.int32) > 0)
        return count + hit, jnp.where(mine, count, rank)

    rank = lax.fori_loop(0, n_ctx, source,
                         (jnp.int32(0), jnp.full((1, n_ctx * blk), -1, jnp.int32)))[1]
    out_row = lax.broadcasted_iota(jnp.int32, (rows, 1), 0)
    rmat[...] = jnp.where(
        (out_row // blk == rank) & (out_row % blk == slot_lane % blk), 1.0, 0.0
    ).astype(jnp.bfloat16)

    scale = math.log2(math.e) / math.sqrt(hd)
    half = rows // 2
    asent = []

    span = 2 * rows
    places = jnp.concatenate([lane_place, lane_place + rows], axis=1)
    mbuf[...] = jnp.full(mbuf.shape, NEG_FILL, jnp.float32)

    def score(chunk, d, carry):
        first = ((me - core + n_ctx - 2 * d) % n_ctx) * rows
        key_place = places + first
        allowed = (key_place >= row_start) & (key_place <= row_place)
        keys = kvwin[pl.ds(pl.multiple_of(d * span, span), span), 0:hd]
        for h in range(chunk * HEAD_CHUNK, (chunk + 1) * HEAD_CHUNK):
            s = lax.dot_general(qbuf[h], keys, (((1,), (1,)), ((), ())),
                                preferred_element_type=jnp.float32)
            s = jnp.where(allowed, s, NEG_FILL)
            sbuf[h, d] = s
            m = mbuf[h]
            for j in range(span // 128):
                m = jnp.maximum(m, s[:, j * 128:(j + 1) * 128])
            mbuf[h] = m
        return carry

    def finish(chunk):
        def one(index, carry):
            c = index // 2
            h = chunk * HEAD_CHUNK + c
            at = pl.ds(pl.multiple_of((index % 2) * half, half), half)
            top = jnp.max(mbuf[h, at, :], axis=1, keepdims=True)
            total = jnp.zeros((half, 128), jnp.float32)
            acc = jnp.zeros((half, hd), jnp.float32)
            for d in range(reach + 1):
                w = jnp.exp2((sbuf[h, d, at, :] - top) * scale)
                for j in range(span // 128):
                    total = total + w[:, j * 128:(j + 1) * 128]
                acc = acc + jnp.dot(w.astype(jnp.bfloat16),
                                    kvwin[d * span:(d + 1) * span, hd:2 * hd],
                                    preferred_element_type=jnp.float32)
            value = acc / jnp.sum(total, axis=1, keepdims=True)
            obuf[c, at, :] = value.astype(jnp.bfloat16)
            return carry

        lax.fori_loop(0, 2 * HEAD_CHUNK, one, 0)

    wide = HEAD_CHUNK * hd

    def a_copy(chunk, d):
        target = (me + d) % n_ctx
        return pltpu.make_async_remote_copy(
            src_ref=sendbuf.at[chunk, pl.ds(pl.multiple_of(target * blk, blk), blk), :],
            dst_ref=recvbuf.at[chunk, pl.ds(pl.multiple_of(me * blk, blk), blk), :],
            send_sem=asend.at[chunk * n_ctx + d], recv_sem=arecv.at[chunk * n_ctx + d],
            device_id={"ctx": target}, device_id_type=MESH)

    def a_got(chunk, d):
        source = (me + n_ctx - d) % n_ctx
        where = recvbuf.at[chunk, pl.ds(pl.multiple_of(source * blk, blk), blk), :]
        pltpu.make_async_remote_copy(
            src_ref=where, dst_ref=where,
            send_sem=asend.at[chunk * n_ctx + d], recv_sem=arecv.at[chunk * n_ctx + d],
            device_id={"ctx": source}, device_id_type=MESH).wait_recv()

    chunks = heads // HEAD_CHUNK
    my_slot = pl.ds(pl.multiple_of(me * blk, blk), blk)
    for chunk in range(chunks):
        lax.fori_loop(0, reach + 1, functools.partial(score, chunk), 0)
        finish(chunk)
        for c in range(HEAD_CHUNK):
            sendbuf[chunk, :, c * hd:(c + 1) * hd] = jnp.dot(
                pmat[...], obuf[c], preferred_element_type=jnp.float32).astype(jnp.bfloat16)

        if chunk == 0:
            pl.semaphore_wait(barrier, n_ctx - 1)

        def go(d, carry):
            a_copy(chunk, d).start()
            return carry

        lax.fori_loop(1, n_ctx, go, 0)
        recvbuf[chunk, my_slot, :] = sendbuf[chunk, my_slot, :]

    for chunk in range(chunks):
        def arrived(d, carry):
            a_got(chunk, d)
            return carry

        lax.fori_loop(1, n_ctx, arrived, 0)
        out_ref[:, chunk * wide:(chunk + 1) * wide] = jnp.dot(
            rmat[...], recvbuf[chunk], preferred_element_type=jnp.float32).astype(jnp.bfloat16)

    for chunk in range(chunks):
        def gone(d, carry):
            a_copy(chunk, d).wait_send()
            return carry

        lax.fori_loop(1, n_ctx, gone, 0)


def body(tokens, query_weight, keyval_weight, doc_lengths, owners):
    n_ctx = lax.axis_size("ctx")
    n_tp = lax.axis_size("tp")
    n_x = n_tp // 2
    share, depth = tokens.shape
    rows = share * n_tp
    hd = keyval_weight.shape[1] // 2
    heads = query_weight.shape[1] // hd
    per_dev = owners.shape[0] // n_ctx
    blk = rows // per_dev
    reach = -(-DOC_MOST // (2 * rows))
    n_docs = doc_lengths.shape[0]
    cfg = (n_ctx, n_x, reach, rows, share, depth, heads, hd, blk, n_docs)
    part = depth // PIECES
    slots = 2 * (reach + 1)
    chunks = heads // HEAD_CHUNK
    wide = HEAD_CHUNK * hd
    bf, f32 = jnp.bfloat16, jnp.float32
    n_tok = 10 * PIECES
    n_kv = 4 * (2 * reach + 1)
    dma = pltpu.SemaphoreType.DMA
    q, kv = pl.pallas_call(
        functools.partial(gather_kernel, cfg),
        out_shape=(jax.ShapeDtypeStruct((heads, rows, hd), bf),
                   jax.ShapeDtypeStruct((slots * rows, 2 * hd), bf)),
        in_specs=[pl.BlockSpec(memory_space=pl.ANY)] * 3,
        out_specs=[pl.BlockSpec(memory_space=pltpu.VMEM)] * 2,
        scratch_shapes=[
            pltpu.VMEM((PIECES, rows, part), bf),
            pltpu.VMEM((PIECES, part, heads * hd), bf),
            pltpu.VMEM((PIECES, part, 2 * hd), bf),
            [pltpu.VMEM((2, rows, 2 * hd), bf) for _ in range(reach + 1)],
            dma((PIECES,)),
            dma((2 * PIECES,)),
            dma((n_tok,)),
            dma((2 * n_x * PIECES,)),
            dma((n_kv,)),
            dma((slots * 4,)),
        ],
        compiler_params=pltpu.CompilerParams(
            collective_id=0, has_side_effects=True, vmem_limit_bytes=48 * 1024 * 1024
        ),
    )(tokens, query_weight, keyval_weight)
    return pl.pallas_call(
        functools.partial(attend_kernel, cfg),
        out_shape=jax.ShapeDtypeStruct((rows, heads * hd), bf),
        in_specs=[pl.BlockSpec(memory_space=pltpu.VMEM)] * 2
        + [pl.BlockSpec(memory_space=pltpu.SMEM)] * 2,
        out_specs=pl.BlockSpec(memory_space=pltpu.VMEM),
        scratch_shapes=[
            pltpu.VMEM((heads, reach + 1, rows, 2 * rows), f32),
            pltpu.VMEM((heads, rows, 128), f32),
            pltpu.VMEM((HEAD_CHUNK, rows, hd), bf),
            pltpu.VMEM((chunks, n_ctx * blk, wide), bf),
            pltpu.VMEM((chunks, n_ctx * blk, wide), bf),
            pltpu.VMEM((n_ctx * blk, rows), bf),
            pltpu.VMEM((rows, n_ctx * blk), bf),
            dma((chunks * n_ctx,)),
            dma((chunks * n_ctx,)),
        ],
        compiler_params=pltpu.CompilerParams(
            collective_id=1, has_side_effects=True, vmem_limit_bytes=48 * 1024 * 1024
        ),
    )(q, kv, doc_lengths, owners)


def solution(mesh):
    return jax.shard_map(
        body,
        mesh=mesh,
        in_specs=(P(("ctx", "tp"), None), P(None, "tp"), P(None, "tp"), P(), P()),
        out_specs=P("ctx", "tp"),
        check_vma=False,
    )
```

```python
import functools
import math

import jax
import jax.numpy as jnp
from jax import lax
from jax.experimental import pallas as pl
from jax.experimental.pallas import tpu as pltpu
from jax.sharding import PartitionSpec as P

NEG_FILL = -1e30
DOC_MOST = 2048
MESH = pl.DeviceIdType.MESH
PIECES = 4
X_FIRST = (0, 1)
Y_FIRST = (2, 3)
GO_RIGHT = (0, 2)
GO_LEFT = (1, 3)
HEAD_CHUNK = 2


def gather_kernel(cfg, tok_hbm, qw_hbm, kw_hbm, q_out, kv_out,
                  tok, wq, wk, kvs, load_sem, w_sem, tsend, trecv, ksend, krecv):
    n_ctx, n_x, reach, rows, share, depth, heads, hd, blk, n_docs = cfg
    me = lax.axis_index("ctx")
    g = lax.axis_index("tp")
    y = g // n_x
    x = g % n_x
    core = me % 2
    xr = (x + 1) % n_x
    xl = (x + n_x - 1) % n_x
    xo = (x + 2) % n_x
    yo = 1 - y
    chunk_rows = 2 * share
    part = depth // PIECES

    def shard_rows(yy, xx):
        return pl.ds(pl.multiple_of((xx * 2 + yy) * share, share), share)

    def group(yy, xx):
        return yy * n_x + xx

    loads = []
    for p in range(PIECES):
        c = pltpu.make_async_copy(tok_hbm.at[:, pl.ds(p * part, part)],
                                  tok.at[p, shard_rows(y, x), :], load_sem.at[p])
        c.start()
        loads.append(c)
    wloads = []
    for p in range(PIECES):
        c = pltpu.make_async_copy(kw_hbm.at[pl.ds(p * part, part), :], wk.at[p], w_sem.at[p])
        c.start()
        wloads.append(c)
        c = pltpu.make_async_copy(qw_hbm.at[pl.ds(p * part, part), :], wq.at[p],
                                  w_sem.at[PIECES + p])
        c.start()
        wloads.append(c)

    barrier = pltpu.get_barrier_semaphore()
    for gg in (group(y, xr), group(y, xl), group(yo, x)):
        pl.semaphore_signal(barrier, inc=1, device_id={"tp": gg}, device_id_type=MESH)

    for cc in ((me + 2) % n_ctx, (me + n_ctx - 2) % n_ctx, me + 1 - 2 * core):
        pl.semaphore_signal(barrier, inc=1, device_id={"ctx": cc}, device_id_type=MESH)
    pl.semaphore_wait(barrier, 6)
    for c in loads:
        c.wait()

    sent = []

    def tok_copy(gg, yy, xx, p, sem):
        where = tok.at[p, shard_rows(yy, xx), :]
        return pltpu.make_async_remote_copy(
            src_ref=where, dst_ref=where, send_sem=tsend.at[sem],
            recv_sem=trecv.at[(xx * 2 + yy) * PIECES + p],
            device_id={"tp": gg}, device_id_type=MESH)

    def send(gg, yy, xx, p):
        c = tok_copy(gg, yy, xx, p, len(sent))
        c.start()
        sent.append(c)

    def got(yy, xx, p):
        tok_copy(g, yy, xx, p, 0).wait_recv()

    right, left, over = group(y, xr), group(y, xl), group(yo, x)
    for p in Y_FIRST + X_FIRST:
        send(over, y, x, p)
    for p in X_FIRST + Y_FIRST:
        send(right, y, x, p)
        send(left, y, x, p)

    for d in range(1, reach + 1):
        def clear(d=d):
            kvs[d][...] = jnp.zeros(kvs[d].shape, jnp.bfloat16)
        pl.when(me // 2 < d)(clear)

    ksent = []
    chunk_x = (x, xl, xr, xo)

    def chunk_at(k):
        return pl.ds(pl.multiple_of(chunk_x[k] * chunk_rows, chunk_rows), chunk_rows)

    def kv_copy(target, src_d, dst_d, half, k, sem):
        return pltpu.make_async_remote_copy(
            src_ref=kvs[src_d].at[half, chunk_at(k), :],
            dst_ref=kvs[dst_d].at[half, chunk_at(k), :],
            send_sem=ksend.at[sem], recv_sem=krecv.at[dst_d * 8 + half * 4 + k],
            device_id={"ctx": target}, device_id_type=MESH)

    def kv_send(target, src_d, dst_d, k, when):
        c = kv_copy(target, src_d, dst_d, core, k, len(ksent))
        pl.when(when)(c.start)
        ksent.append((c, when))

    def kv_got(d, half, k):
        kv_copy(me, d, d, half, k, 0).wait_recv()

    up = (me + 2) % n_ctx
    twin = me + 1 - 2 * core
    chip = me // 2
    last = n_ctx // 2 - 1

    def kv_step(step):
        for d in range(0, reach + 1):
            k = step - d
            if k < 0 or k > 3:
                continue
            if d > 0:
                pl.when(chip >= d)(functools.partial(kv_got, d, core, k))
            if d < reach:
                kv_send(up, d, d + 1, k, (chip >= d) & (chip < last))
            kv_send(twin, d, d, k, chip >= d)

    def project(k):
        at = chunk_at(k)

        def kv_part(p, acc):
            return acc + jnp.dot(tok[p, at, :], wk[p], preferred_element_type=jnp.float32)

        kv = lax.fori_loop(0, PIECES, kv_part, jnp.zeros((chunk_rows, 2 * hd), jnp.float32))
        kvs[0][core, at, :] = kv.astype(jnp.bfloat16)
        kv_step(k)

        def q_part(p, acc):
            return acc + jnp.dot(tok[p, at, :], wq[p], preferred_element_type=jnp.float32)

        q = lax.fori_loop(0, PIECES, q_part, jnp.zeros((chunk_rows, heads * hd), jnp.float32))
        q = q.astype(jnp.bfloat16)
        for h in range(heads):
            q_out[h, at, :] = q[:, h * hd:(h + 1) * hd]

    for p in Y_FIRST:
        got(yo, x, p)
        send(right, yo, x, p)
        send(left, yo, x, p)
    for p in X_FIRST:
        got(y, xl, p)
        if p in GO_RIGHT:
            send(right, y, xl, p)
        send(over, y, xl, p)
        got(y, xr, p)
        if p in GO_LEFT:
            send(left, y, xr, p)
        send(over, y, xr, p)
    for c in wloads:
        c.wait()
    for p in X_FIRST:
        got(yo, x, p)
    project(0)
    for p in Y_FIRST:
        got(y, xl, p)
        if p in GO_RIGHT:
            send(right, y, xl, p)
        got(y, xr, p)
        if p in GO_LEFT:
            send(left, y, xr, p)
    for p in X_FIRST:
        got(y, xo, p)
        send(over, y, xo, p)
    for p in Y_FIRST:
        got(yo, xl, p)
        if p in GO_RIGHT:
            send(right, yo, xl, p)
        got(yo, xr, p)
        if p in GO_LEFT:
            send(left, yo, xr, p)
    for p in X_FIRST:
        got(yo, xl, p)
    project(1)
    for p in X_FIRST:
        got(yo, xr, p)
    project(2)
    for p in Y_FIRST:
        got(y, xo, p)
    for p in X_FIRST:
        got(yo, xo, p)
    for p in Y_FIRST:
        got(yo, xo, p)
    project(3)

    def twin_got(d):
        for k in range(4):
            kv_got(d, 1 - core, k)

    for d in range(reach + 1):
        if d > 0:
            kv_step(3 + d)
        pl.when(chip >= d)(functools.partial(twin_got, d))
        for half in range(2):
            kv_out[(2 * d + half) * rows:(2 * d + half + 1) * rows, :] = kvs[d][half]
    for c in sent:
        c.wait_send()
    for c, when in ksent:
        pl.when(when)(c.wait_send)


def attend_kernel(cfg, qbuf, kvwin, doc_ref, own_ref, out_ref,
                  sbuf, mbuf, obuf, sendbuf, recvbuf, pmat, rmat, asend, arecv):
    n_ctx, n_x, reach, rows, share, depth, heads, hd, blk, n_docs = cfg
    me = lax.axis_index("ctx")
    core = me % 2
    chunk_rows = 2 * share
    per_dev = rows // blk
    barrier = pltpu.get_barrier_semaphore()

    def greet(d, carry):
        pl.semaphore_signal(barrier, inc=1, device_id={"ctx": (me + d) % n_ctx},
                            device_id_type=MESH)
        return carry

    lax.fori_loop(1, n_ctx, greet, 0)

    def place(index):
        return ((index // share) % 2) * (n_x * share) + (index // chunk_rows) * share + index % share

    row_place = me * rows + place(lax.broadcasted_iota(jnp.int32, (rows, 1), 0))

    def next_doc(d, carry):
        end, start = carry
        end = end + doc_ref[d]
        return end, jnp.where(row_place >= end, end, start)

    row_start = lax.fori_loop(0, n_docs, next_doc,
                              (jnp.int32(0), jnp.zeros((rows, 1), jnp.int32)))[1]

    lane_place = place(lax.broadcasted_iota(jnp.int32, (1, rows), 1))

    def block_owner(j, carry):
        return jnp.where(lane_place // blk == j, own_ref[me * per_dev + j], carry)

    lane_owner = lax.fori_loop(0, per_dev, block_owner, jnp.zeros((1, rows), jnp.int32))
    slot_row = lax.broadcasted_iota(jnp.int32, (n_ctx * blk, 1), 0)
    pmat[...] = jnp.where(
        (slot_row // blk == lane_owner) & (slot_row % blk == lane_place % blk), 1.0, 0.0
    ).astype(jnp.bfloat16)
    slot_lane = lax.broadcasted_iota(jnp.int32, (1, n_ctx * blk), 1)

    def source(s, carry):
        count, rank = carry
        hit = jnp.int32(0)
        for j in range(per_dev):
            hit = hit + jnp.where(own_ref[s * per_dev + j] == me, 1, 0)
        mine = (slot_lane // blk == s) & (jnp.full(slot_lane.shape, hit, jnp.int32) > 0)
        return count + hit, jnp.where(mine, count, rank)

    rank = lax.fori_loop(0, n_ctx, source,
                         (jnp.int32(0), jnp.full((1, n_ctx * blk), -1, jnp.int32)))[1]
    out_row = lax.broadcasted_iota(jnp.int32, (rows, 1), 0)
    rmat[...] = jnp.where(
        (out_row // blk == rank) & (out_row % blk == slot_lane % blk), 1.0, 0.0
    ).astype(jnp.bfloat16)

    scale = math.log2(math.e) / math.sqrt(hd)
    half = rows // 2
    asent = []

    span = 2 * rows
    places = jnp.concatenate([lane_place, lane_place + rows], axis=1)
    mbuf[...] = jnp.full(mbuf.shape, NEG_FILL, jnp.float32)

    def score(chunk, d, carry):
        first = ((me - core + n_ctx - 2 * d) % n_ctx) * rows
        key_place = places + first
        allowed = (key_place >= row_start) & (key_place <= row_place)
        keys = kvwin[pl.ds(pl.multiple_of(d * span, span), span), 0:hd]
        for h in range(chunk * HEAD_CHUNK, (chunk + 1) * HEAD_CHUNK):
            s = lax.dot_general(qbuf[h], keys, (((1,), (1,)), ((), ())),
                                preferred_element_type=jnp.float32)
            s = jnp.where(allowed, s, NEG_FILL)
            sbuf[h, d] = s
            m = mbuf[h]
            for j in range(span // 128):
                m = jnp.maximum(m, s[:, j * 128:(j + 1) * 128])
            mbuf[h] = m
        return carry

    def finish(chunk):
        def one(index, carry):
            c = index // 2
            h = chunk * HEAD_CHUNK + c
            at = pl.ds(pl.multiple_of((index % 2) * half, half), half)
            top = jnp.max(mbuf[h, at, :], axis=1, keepdims=True)
            total = jnp.zeros((half, 128), jnp.float32)
            acc = jnp.zeros((half, hd), jnp.float32)
            for d in range(reach + 1):
                w = jnp.exp2((sbuf[h, d, at, :] - top) * scale)
                for j in range(span // 128):
                    total = total + w[:, j * 128:(j + 1) * 128]
                acc = acc + jnp.dot(w.astype(jnp.bfloat16),
                                    kvwin[d * span:(d + 1) * span, hd:2 * hd],
                                    preferred_element_type=jnp.float32)
            value = acc / jnp.sum(total, axis=1, keepdims=True)
            obuf[c, at, :] = value.astype(jnp.bfloat16)
            return carry

        lax.fori_loop(0, 2 * HEAD_CHUNK, one, 0)

    wide = HEAD_CHUNK * hd

    def a_copy(chunk, d):
        target = (me + d) % n_ctx
        return pltpu.make_async_remote_copy(
            src_ref=sendbuf.at[chunk, pl.ds(pl.multiple_of(target * blk, blk), blk), :],
            dst_ref=recvbuf.at[chunk, pl.ds(pl.multiple_of(me * blk, blk), blk), :],
            send_sem=asend.at[chunk * n_ctx + d], recv_sem=arecv.at[chunk * n_ctx + d],
            device_id={"ctx": target}, device_id_type=MESH)

    def a_got(chunk, d):
        source = (me + n_ctx - d) % n_ctx
        where = recvbuf.at[chunk, pl.ds(pl.multiple_of(source * blk, blk), blk), :]
        pltpu.make_async_remote_copy(
            src_ref=where, dst_ref=where,
            send_sem=asend.at[chunk * n_ctx + d], recv_sem=arecv.at[chunk * n_ctx + d],
            device_id={"ctx": source}, device_id_type=MESH).wait_recv()

    chunks = heads // HEAD_CHUNK
    my_slot = pl.ds(pl.multiple_of(me * blk, blk), blk)
    for chunk in range(chunks):
        lax.fori_loop(0, reach + 1, functools.partial(score, chunk), 0)
        finish(chunk)
        for c in range(HEAD_CHUNK):
            sendbuf[chunk, :, c * hd:(c + 1) * hd] = jnp.dot(
                pmat[...], obuf[c], preferred_element_type=jnp.float32).astype(jnp.bfloat16)

        if chunk == 0:
            pl.semaphore_wait(barrier, n_ctx - 1)

        def go(d, carry):
            a_copy(chunk, d).start()
            return carry

        lax.fori_loop(1, n_ctx, go, 0)
        recvbuf[chunk, my_slot, :] = sendbuf[chunk, my_slot, :]

    for chunk in range(chunks):
        def arrived(d, carry):
            a_got(chunk, d)
            return carry

        lax.fori_loop(1, n_ctx, arrived, 0)
        out_ref[:, chunk * wide:(chunk + 1) * wide] = jnp.dot(
            rmat[...], recvbuf[chunk], preferred_element_type=jnp.float32).astype(jnp.bfloat16)

    for chunk in range(chunks):
        def gone(d, carry):
            a_copy(chunk, d).wait_send()
            return carry

        lax.fori_loop(1, n_ctx, gone, 0)


def body(tokens, query_weight, keyval_weight, doc_lengths, owners):
    n_ctx = lax.axis_size("ctx")
    n_tp = lax.axis_size("tp")
    n_x = n_tp // 2
    share, depth = tokens.shape
    rows = share * n_tp
    hd = keyval_weight.shape[1] // 2
    heads = query_weight.shape[1] // hd
    per_dev = owners.shape[0] // n_ctx
    blk = rows // per_dev
    reach = -(-DOC_MOST // (2 * rows))
    n_docs = doc_lengths.shape[0]
    cfg = (n_ctx, n_x, reach, rows, share, depth, heads, hd, blk, n_docs)
    part = depth // PIECES
    slots = 2 * (reach + 1)
    chunks = heads // HEAD_CHUNK
    wide = HEAD_CHUNK * hd
    bf, f32 = jnp.bfloat16, jnp.float32
    n_tok = 10 * PIECES
    n_kv = 4 * (2 * reach + 1)
    dma = pltpu.SemaphoreType.DMA
    q, kv = pl.pallas_call(
        functools.partial(gather_kernel, cfg),
        out_shape=(jax.ShapeDtypeStruct((heads, rows, hd), bf),
                   jax.ShapeDtypeStruct((slots * rows, 2 * hd), bf)),
        in_specs=[pl.BlockSpec(memory_space=pl.ANY)] * 3,
        out_specs=[pl.BlockSpec(memory_space=pltpu.VMEM)] * 2,
        scratch_shapes=[
            pltpu.VMEM((PIECES, rows, part), bf),
            pltpu.VMEM((PIECES, part, heads * hd), bf),
            pltpu.VMEM((PIECES, part, 2 * hd), bf),
            [pltpu.VMEM((2, rows, 2 * hd), bf) for _ in range(reach + 1)],
            dma((PIECES,)),
            dma((2 * PIECES,)),
            dma((n_tok,)),
            dma((2 * n_x * PIECES,)),
            dma((n_kv,)),
            dma((slots * 4,)),
        ],
        compiler_params=pltpu.CompilerParams(
            collective_id=0, has_side_effects=True, vmem_limit_bytes=48 * 1024 * 1024
        ),
    )(tokens, query_weight, keyval_weight)
    return pl.pallas_call(
        functools.partial(attend_kernel, cfg),
        out_shape=jax.ShapeDtypeStruct((rows, heads * hd), bf),
        in_specs=[pl.BlockSpec(memory_space=pltpu.VMEM)] * 2
        + [pl.BlockSpec(memory_space=pltpu.SMEM)] * 2,
        out_specs=pl.BlockSpec(memory_space=pltpu.VMEM),
        scratch_shapes=[
            pltpu.VMEM((heads, reach + 1, rows, 2 * rows), f32),
            pltpu.VMEM((heads, rows, 128), f32),
            pltpu.VMEM((HEAD_CHUNK, rows, hd), bf),
            pltpu.VMEM((chunks, n_ctx * blk, wide), bf),
            pltpu.VMEM((chunks, n_ctx * blk, wide), bf),
            pltpu.VMEM((n_ctx * blk, rows), bf),
            pltpu.VMEM((rows, n_ctx * blk), bf),
            dma((chunks * n_ctx,)),
            dma((chunks * n_ctx,)),
        ],
        compiler_params=pltpu.CompilerParams(
            collective_id=1, has_side_effects=True, vmem_limit_bytes=48 * 1024 * 1024
        ),
    )(q, kv, doc_lengths, owners)


def solution(mesh):
    return jax.shard_map(
        body,
        mesh=mesh,
        in_specs=(P(("ctx", "tp"), None), P(None, "tp"), P(None, "tp"), P(), P()),
        out_specs=P("ctx", "tp"),
        check_vma=False,
    )
```
